32 devices in a mesh: ens: 4 (over y, x), slab: 8 (over z, core).
Axes of the slice: x: 2, y: 2, z: 4, core: 2. Of those that a mesh axis runs over, the one named last changes fastest.
Arguments:
- velocity: float32 [4, 3, 8, 2048, 1024], P('ens', None, None, 'slab'), may hold values from -6 to 6
- cutoffs: int32 [4, 2, 8], P('ens'), may hold values from 128 to 511, as said below
- plane_index: int32 [4], P('ens'), may hold values from 0 to 2047
- boundary_index: int32 [4], P('ens'), may hold values from 0 to 2047
Outputs:
- blended: float32 [4, 3, 8, 2048, 1024], P('ens', None, None, 'slab')
The draws below stay inside these ranges and needn't reach their ends.
Inputs may be any that keep to these rules, and one draw needn't show every extreme that they name: `cutoffs`: row 0 lies in 256 to 511 and row 1 in 128 to 255; in every member some level has row 0 equal to 511 and some level has row 1 equal to 255.
All inputs are finite; a program needn't handle non-finite values.
Results may differ from the reference program's by a relative error of at most 0.0003.
Values sent between devices are 32-bit elements; how exact they have to be, the bound alone decides.
A program may use at most 128 MiB of HBM per device.

```python
import jax
import jax.numpy as jnp
from jax import lax

NX = 2048
NY = 1024
KX = 512
KY = 256
COMP = 3
Z = 8
ENS = 4
N_ENS = 4


def draw_cutoffs(key, part):
    key_x, key_y, key_a, key_b = jax.random.split(jax.random.fold_in(key, 17), 4)
    levels = jnp.arange(Z, dtype=jnp.int32)
    cut_x = jax.random.randint(key_x, (N_ENS, Z), KX // 2, KX, dtype=jnp.int32)
    cut_y = jax.random.randint(key_y, (N_ENS, Z), KY // 2, KY, dtype=jnp.int32)
    top_x = jax.random.randint(key_a, (N_ENS, 1), 0, Z, dtype=jnp.int32)
    top_y = jax.random.randint(key_b, (N_ENS, 1), 0, Z, dtype=jnp.int32)
    cut_x = jnp.where(levels[None, :] == top_x, KX - 1, cut_x)
    cut_y = jnp.where(levels[None, :] == top_y, KY - 1, cut_y)
    return jnp.stack([cut_x, cut_y], axis=1).astype(jnp.int32)


def with_ends(values, rng, least, high):
    longest = values.shape.index(max(values.shape))
    spots = []
    for shift in (0, 1):
        where = [jax.random.randint(jax.random.fold_in(rng, axis), (), 0, length) for axis, length in enumerate(values.shape)]
        where[longest] = (where[longest] + shift) % values.shape[longest]
        spots.append(tuple(where))
    return values.at[spots[0]].set(least).at[spots[1]].set(high)


def level_of(stream_key, shape, cuts, low, high):
    gain, own = 1.0, jax.random.fold_in(stream_key, 6)
    for axis_at, blocks in cuts:
        steps = jnp.exp(jax.random.uniform(jax.random.fold_in(own, axis_at), (blocks,), jnp.float32, low / len(cuts), high / len(cuts)))
        gain = gain * jnp.repeat(steps, shape[axis_at] // blocks).reshape([-1 if axis == axis_at else 1 for axis in range(len(shape))])
    return gain


def bell_draw(stream_key, shape, deviation, bound, shards=(), kind=jnp.bfloat16):
    array = deviation * jax.random.normal(stream_key, shape, jnp.float32)
    if shards:
        array = array * level_of(stream_key, shape, shards, -0.22, 0.18)
    return jnp.clip(array, -bound, bound).astype(kind)


def setup_inputs(seed: int = 0) -> dict:
    splits = jax.random.split(jax.random.key(seed), 5)
    velocity = bell_draw(splits[0], (ENS, COMP, Z, NX, NY), 1.0, 6.0, ((0, 4), (3, 8)), jnp.float32)
    cutoffs = draw_cutoffs(jax.random.fold_in(splits[4], 71), 0)
    plane_index = with_ends(jax.random.randint(splits[2], (ENS,), 0, NX), jax.random.fold_in(splits[2], 1), 0, NX - 1).astype(jnp.int32)
    boundary_index = with_ends(jax.random.randint(splits[3], (ENS,), 0, NX), jax.random.fold_in(splits[3], 1), 0, NX - 1).astype(jnp.int32)
    return dict(velocity=velocity, cutoffs=cutoffs, plane_index=plane_index, boundary_index=boundary_index)


def filter_one(member_item):
    grid_values, cut_x, cut_y = member_item
    spectrum = jnp.fft.fft2(grid_values)
    wave_x = jnp.arange(NX, dtype=jnp.int32)
    wave_y = jnp.arange(NY, dtype=jnp.int32)
    kabs_x = jnp.minimum(wave_x, NX - wave_x)
    kabs_y = jnp.minimum(wave_y, NY - wave_y)
    keep = (kabs_x[:, None] <= cut_x) & (kabs_y[None, :] <= cut_y)
    kept = jnp.where(keep, spectrum, jnp.zeros_like(spectrum))
    return jnp.real(jnp.fft.ifft2(kept)).astype(grid_values.dtype)


def pick_plane(member_field, index_value):
    return lax.dynamic_index_in_dim(member_field, index_value.astype(jnp.int32), 2, keepdims=False)


def reference(velocity, cutoffs, plane_index, boundary_index):
    stacked = velocity.reshape(-1, NX, NY)
    cut_x = jnp.broadcast_to(cutoffs[:, 0][:, None, :], (N_ENS, COMP, Z)).reshape(-1)
    cut_y = jnp.broadcast_to(cutoffs[:, 1][:, None, :], (N_ENS, COMP, Z)).reshape(-1)
    filtered = lax.map(filter_one, (stacked, cut_x, cut_y)).reshape(velocity.shape)
    planes = jax.vmap(pick_plane)(filtered, plane_index)
    inflow = jnp.roll(planes, 1, axis=0)
    streamwise = jnp.arange(NX, dtype=jnp.int32)
    offset = jnp.abs(streamwise[None, :] - boundary_index.astype(jnp.int32)[:, None])
    distance = jnp.minimum(offset, NX - offset)
    relax = jnp.exp(-distance.astype(filtered.dtype) / (NX / 4.0))
    weight = relax[:, None, None, :, None]
    return filtered + weight * (inflow[:, :, :, None, :] - filtered)
```

```python
import functools
import math

import jax
import jax.numpy as jnp
from jax import lax
from jax.experimental import pallas as pl
from jax.experimental.pallas import tpu as pltpu
from jax.sharding import PartitionSpec as P

KX = 512
KY = 256
CHUNK = 4

f32 = jnp.float32
bf16 = jnp.bfloat16

NN = (((1,), (0,)), ((), ()))
NT = (((1,), (1,)), ((), ()))


def halves(value):
    high = value.astype(bf16)
    return high, (value - high.astype(f32)).astype(bf16)


def table_halves(value):
    high = lax.reduce_precision(value, 8, 7)
    return high.astype(bf16), (value - high).astype(bf16)


def dot3(left, right, dims):
    (lh, ll), (rh, rl) = left, right
    dot = functools.partial(lax.dot_general, dimension_numbers=dims, preferred_element_type=f32)
    return dot(lh, rh) + (dot(ll, rh) + dot(lh, rl))


def analyse_y_kernel(field, bh, bl, out):
    devices, _, width, rows = out.shape
    coeffs = dot3((bh[...], bl[...]), halves(field[0]), NT)
    out[...] = coeffs.reshape(devices, 1, width, rows)


def analyse_x_kernel(lines, ch, cl, fx, fy, out):
    devices, planes, width, rows = lines.shape
    total = None
    for d in range(devices):
        part = dot3(
            halves(lines[d].reshape(planes * width, rows)),
            (ch[pl.ds(d * rows, rows), :], cl[pl.ds(d * rows, rows), :]),
            NN,
        )
        total = part if total is None else total + part
    out[...] = total.reshape(planes, width, -1) * fx[...] * fy[...]


def synthesise_x_kernel(spectra, ch, cl, relax, inflow, out):
    planes, width, modes = spectra.shape
    smooth = dot3(halves(spectra[...].reshape(planes * width, modes)), (ch[...], cl[...]), NT)
    smooth = smooth.reshape(planes, width, -1)
    out[0] = smooth + relax[0][None] * (inflow[...] - smooth)


def synthesise_y_kernel(coeffs, bh, bl, *refs):
    out = refs[-1]
    devices, _, width, rows = coeffs.shape
    lines = coeffs[...].reshape(devices * width, rows).T
    out[0] = dot3(halves(lines), (bh[...], bl[...]), NN)


def cost(flops, nbytes):
    return pl.CostEstimate(flops=int(flops), bytes_accessed=int(nbytes), transcendentals=0)


def params(n):
    return pltpu.CompilerParams(dimension_semantics=("arbitrary",) * n, vmem_limit_bytes=60 * 2**20)


def waves(wavenum, position, length):
    angles = (wavenum * position % length).astype(f32) * (2.0 * math.pi / length)
    return angles


def weights(mode_count, length):
    wavenum = jnp.arange(mode_count, dtype=jnp.int32)
    weight = jnp.where(wavenum == 0, 1.0, 2.0).astype(f32) / length
    return jnp.concatenate([weight, weight])


def on_device(velocity, cutoffs, plane_index, boundary_index):
    devices = lax.axis_size("slab")
    members = lax.axis_size("ens")
    me = lax.axis_index("slab")
    comps, levels, rows, across = velocity.shape[1:]
    along = rows * devices
    planes = comps * levels
    jtot, ktot = 2 * KY, 2 * KX
    width = jtot // devices
    size = CHUNK
    field = velocity.reshape(planes, rows, across)

    ky = jnp.arange(KY, dtype=jnp.int32)
    ang_y = waves(ky[:, None], jnp.arange(across, dtype=jnp.int32)[None, :], across)
    bh, bl = table_halves(jnp.concatenate([jnp.cos(ang_y), jnp.sin(ang_y)], axis=0))
    kx = jnp.arange(KX, dtype=jnp.int32)
    ang_x = waves(jnp.arange(along, dtype=jnp.int32)[:, None], kx[None, :], along)
    ch, cl = table_halves(jnp.concatenate([jnp.cos(ang_x), jnp.sin(ang_x)], axis=1))

    kx2 = jnp.tile(kx, 2)
    fx = (kx2[None, :] <= cutoffs[0, 0][:, None]).astype(f32) * weights(KX, along)[None]
    fx = jnp.tile(fx, (comps, 1))[:, None, :]
    fy = (jnp.tile(ky, 2)[None, :] <= cutoffs[0, 1][:, None]).astype(f32) * weights(KY, across)[None]
    fy = lax.dynamic_slice_in_dim(fy, me * width, width, 1)
    fy = jnp.tile(fy, (comps, 1))[:, :, None]

    ang_p = waves(plane_index[0], kx, along)
    at_plane = jnp.concatenate([jnp.cos(ang_p), jnp.sin(ang_p)])
    offset = jnp.abs(jnp.arange(along, dtype=jnp.int32) - boundary_index[0])
    distance = jnp.minimum(offset, along - offset)
    relax = jnp.exp(-distance.astype(f32) / (along / 4.0)).reshape(devices, 1, rows)

    kblock = 256
    route = [((i - 1) % members, i) for i in range(members)]
    sends = []
    for g in range(planes // size):
        first = g * size
        sends.append(
            pl.pallas_call(
                analyse_y_kernel,
                grid=(size,),
                in_specs=[
                    pl.BlockSpec((1, rows, across), lambda i, first=first: (first + i, 0, 0)),
                    pl.BlockSpec((jtot, across), lambda i: (0, 0)),
                    pl.BlockSpec((jtot, across), lambda i: (0, 0)),
                ],
                out_specs=pl.BlockSpec((devices, 1, width, rows), lambda i: (0, i, 0, 0)),
                out_shape=jax.ShapeDtypeStruct((devices, size, width, rows), f32),
                cost_estimate=cost(6 * size * rows * across * jtot, 6 * size * rows * across),
                compiler_params=params(1),
                name="analyse_y",
            )(field, bh, bl)
        )
    lines = [lax.all_to_all(s, "slab", 0, 0, tiled=True) for s in sends]

    backs = []
    for g, got in enumerate(lines):
        first = g * size
        spectra = pl.pallas_call(
            analyse_x_kernel,
            grid=(ktot // kblock,),
            in_specs=[
                pl.BlockSpec((devices, size, width, rows), lambda k: (0, 0, 0, 0)),
                pl.BlockSpec((along, kblock), lambda k: (0, k)),
                pl.BlockSpec((along, kblock), lambda k: (0, k)),
                pl.BlockSpec((size, 1, kblock), lambda k: (0, 0, k)),
                pl.BlockSpec((size, width, 1), lambda k: (0, 0, 0)),
            ],
            out_specs=pl.BlockSpec((size, width, kblock), lambda k: (0, 0, k)),
            out_shape=jax.ShapeDtypeStruct((size, width, ktot), f32),
            cost_estimate=cost(6 * size * width * along * ktot, 4 * size * width * along + 4 * along * ktot),
            compiler_params=params(1),
            name="analyse_x",
        )(got, ch, cl, fx[first : first + size], fy[first : first + size])
        handed = jnp.sum(spectra * at_plane, axis=-1)
        inflow = lax.ppermute(handed, "ens", route)[:, :, None]
        smooth = pl.pallas_call(
            synthesise_x_kernel,
            grid=(devices,),
            in_specs=[
                pl.BlockSpec((size, width, ktot), lambda d: (0, 0, 0)),
                pl.BlockSpec((rows, ktot), lambda d: (d, 0)),
                pl.BlockSpec((rows, ktot), lambda d: (d, 0)),
                pl.BlockSpec((1, 1, rows), lambda d: (d, 0, 0)),
                pl.BlockSpec((size, width, 1), lambda d: (0, 0, 0)),
            ],
            out_specs=pl.BlockSpec((1, size, width, rows), lambda d: (d, 0, 0, 0)),
            out_shape=jax.ShapeDtypeStruct((devices, size, width, rows), f32),
            cost_estimate=cost(6 * size * width * along * ktot, 4 * size * width * along + 4 * along * ktot),
            compiler_params=params(1),
            name="synthesise_x",
        )(spectra, ch, cl, relax, inflow)
        backs.append(lax.all_to_all(smooth, "slab", 0, 0, tiled=True))

    result = None
    for g, back in enumerate(backs):
        first = g * size
        extra = [] if result is None else [result]
        result = pl.pallas_call(
            synthesise_y_kernel,
            grid=(size,),
            in_specs=[
                pl.BlockSpec((devices, 1, width, rows), lambda i: (0, i, 0, 0)),
                pl.BlockSpec((jtot, across), lambda i: (0, 0)),
                pl.BlockSpec((jtot, across), lambda i: (0, 0)),
            ]
            + [pl.BlockSpec(memory_space=pl.ANY)] * len(extra),
            out_specs=pl.BlockSpec((1, rows, across), lambda i, first=first: (first + i, 0, 0)),
            out_shape=jax.ShapeDtypeStruct((planes, rows, across), f32),
            input_output_aliases={3: 0} if extra else {},
            cost_estimate=cost(6 * size * rows * across * jtot, 6 * size * rows * across),
            compiler_params=params(1),
            name="synthesise_y",
        )(back, bh, bl, *extra)
    return result.reshape(velocity.shape)


def solution(mesh):
    in_specs = (P("ens", None, None, "slab", None), P("ens", None, None), P("ens"), P("ens"))
    out_specs = P("ens", None, None, "slab", None)
    return jax.shard_map(
        on_device, mesh=mesh, in_specs=in_specs, out_specs=out_specs, check_vma=False
    )
```
